32 devices in a mesh: grp: 4 (over x, core), dev: 8 (over z, y).
Axes of the slice: x: 2, y: 2, z: 4, core: 2. Of those that a mesh axis runs over, the one named last changes fastest.
Arguments:
- points: bfloat16 [65536, 1024], P(('grp', 'dev')), may hold values from -6 to 6
- blocks: int32 [65536, 1], P(('grp', 'dev')), may hold values from 0 to 63; in each aligned block of 2048 rows (0 to 2047, 2048 to 4095, ...) at most 64 rows name the same one
- finals: int32 [65536], P(('grp', 'dev')), may hold values from 0 to 255
- centroids: bfloat16 [16384, 1024], P('dev'), may hold values from -6 to 6
Outputs:
- distances: bfloat16 [65536, 256], P(('grp', 'dev'))
- refreshed_centroids: float32 [16384, 1024], P('dev', 'grp')
The draws below stay inside these ranges and needn't reach their ends.
Inputs may be any that keep to these rules, and one draw needn't show every extreme that they name: `blocks`: among the 2048 rows of one device no block is named by more than 64 rows, and some block by exactly 64. Block b is held by index b // 8 of dev. The point's centroid is row 256 * blocks + finals of centroids.
All inputs are finite; a program needn't handle non-finite values.
Results may differ from the reference program's by a relative error of at most 0.008.
Values may be sent and summed in bfloat16 or wider, within the bound.
A program may use at most 128 MiB of HBM per device.

```python
import math
import jax
import jax.numpy as jnp
import numpy as np
from jax import lax

D = 1024
BS = 256
POINTS_PER_SHARD = 2048
NB = 64
K = 16384
P_SIZE = 65536
MOST = 64
N_GRP = 4
N_DEV = 8


def place_ends(entries, own_key, smallest, top_value):
    dims = entries.shape
    index_at = [jax.random.randint(jax.random.fold_in(own_key, axis), (), 0, dims[axis]) for axis in range(len(dims))]
    entries = entries.at[tuple(index_at)].set(smallest)
    longest = dims.index(max(dims))
    index_at[longest] = (index_at[longest] + 1) % dims[longest]
    return entries.at[tuple(index_at)].set(top_value)


def shard_levels(stream_key, extent, cuts, smallest, top_value):
    def one(position, blocks):
        steps = jax.random.uniform(jax.random.fold_in(jax.random.fold_in(stream_key, 6), position), (blocks,), jnp.float32, smallest / len(cuts), top_value / len(cuts))
        return jnp.repeat(jnp.exp(steps), extent[position] // blocks).reshape((-1,) + (1,) * (len(extent) - position - 1))

    loudness = one(*cuts[0])
    for cut in cuts[1:]:
        loudness = loudness * one(*cut)
    return loudness


def assign_block(key, own, number, rows, count, top, most, skew):
    ranking = jax.random.permutation(key, count)
    heavy_load, usual = load_shares(count, rows * top, most, skew, True), load_shares(count, rows * top, most, skew, False)
    places = jnp.arange(count)

    def named(sizes, offset_by):
        used = int((sizes > 0).sum())
        fixed = max(1, used // 4)
        shifted = fixed + (places - fixed + offset_by * (used - fixed)) % max(1, count - fixed)
        return jnp.zeros((count,), jnp.int32).at[ranking[jnp.where(places < fixed, places, shifted)]].set(jnp.asarray(sizes, jnp.int32))

    sizes = jnp.where(number % 4 == 0, named(heavy_load, number // 4), named(usual, number - number // 4 - 1))
    mixed = jax.random.permutation(jax.random.fold_in(own, 3), count)
    giver, taker = mixed[0:count // 2 * 2:2], mixed[1:count // 2 * 2:2]
    margin = jnp.minimum(sizes[giver] - 1, most - sizes[taker]) // 2
    margin = jnp.where((giver == ranking[0]) | (taker == ranking[0]) | (sizes[taker] == 0), 0, jnp.maximum(margin, 0))
    shifted = jax.random.randint(jax.random.fold_in(own, 4), (count // 2,), 0, 1 << 20) % (margin + 1)
    sizes = sizes.at[giver].add(-shifted).at[taker].add(shifted)
    items = jnp.searchsorted(jnp.cumsum(sizes), jnp.arange(rows * top), side="right").astype(jnp.int32)
    grid = items.reshape(top, rows).T
    grid = grid[jax.random.permutation(jax.random.fold_in(own, 1), rows)]
    offset_by = jax.random.randint(jax.random.fold_in(own, 2), (rows, 1), 0, top)
    return jnp.take_along_axis(grid, (jnp.arange(top)[None, :] + offset_by) % top, axis=1)


def load_shares(amount, total, limit, slope, full):
    loads = [(1 << 20) // math.isqrt(rank ** slope) + 1 for rank in range(1, amount + 1)]
    largest = limit if full else min(limit, max(-(-total // amount), total * loads[0] // sum(loads)))
    least = 1 if total - largest >= amount - 1 else 0
    holding, surplus = [largest] + [least] * (amount - 1), total - largest - least * (amount - 1)
    while surplus > 0:
        free = [i for i in range(1, amount) if holding[i] < largest] or [i for i in range(1, amount) if holding[i] < limit]
        mass, left = sum([loads[i] for i in free]), surplus
        for i in free:
            extra = min(limit - holding[i], max(1, left * loads[i] // mass), surplus)
            holding[i] = holding[i] + extra
            surplus = surplus - extra
    return np.array(holding)


def normal_values(stream_key, dims, scale, bound, pieces=(), held_as=jnp.bfloat16):
    gain = shard_levels(stream_key, dims, pieces, -0.22, 0.18) if pieces else 1.0
    values = jax.random.normal(stream_key, dims, jnp.float32) * scale * gain
    return jnp.minimum(jnp.maximum(values, -bound), bound).astype(held_as)


def setup_inputs(seed: int = 0) -> dict:
    key_list = jax.random.split(jax.random.key(seed), 5)
    points = normal_values(key_list[0], (P_SIZE, D), 1.0, 6.0, ((0, 32),))
    blocks_keys = jax.random.split(jax.random.fold_in(key_list[1], 1), P_SIZE // POINTS_PER_SHARD)
    blocks_turns = jax.random.permutation(jax.random.fold_in(key_list[1], 3), P_SIZE // POINTS_PER_SHARD)
    blocks = jax.vmap(lambda own, number: assign_block(jax.random.fold_in(key_list[1], 2), own, number, POINTS_PER_SHARD, NB, 1, MOST, 2))(blocks_keys, blocks_turns).reshape((P_SIZE, 1))
    finals = place_ends(jax.random.randint(key_list[2], (P_SIZE,), 0, BS), jax.random.fold_in(key_list[2], 1), 0, BS - 1).astype(jnp.int32)
    centroids = normal_values(key_list[3], (K, D), 1.0, 6.0, ((0, 8),))
    return {"points": points, "blocks": blocks, "finals": finals, "centroids": centroids}


def reference(points, blocks, finals, centroids):
    npoints, width = points.shape
    nblocks = centroids.shape[0] // BS
    reach = N_GRP * N_DEV * MOST
    block_ids = blocks[:, 0].astype(jnp.int32)
    order = jnp.argsort(block_ids, stable=True).astype(jnp.int32)
    ordered = block_ids[order]
    labels = jnp.arange(nblocks, dtype=jnp.int32)
    starts = jnp.searchsorted(ordered, labels, side="left").astype(jnp.int32)
    stops = jnp.searchsorted(ordered, labels, side="right").astype(jnp.int32)
    padded = jnp.concatenate([order, jnp.zeros((reach,), jnp.int32)])
    columns = jnp.arange(BS, dtype=jnp.int32)
    positions = jnp.arange(reach, dtype=jnp.int32)

    def one_block(label):
        begin = starts[label]
        chosen = lax.dynamic_slice_in_dim(padded, begin, reach)
        live = positions < (stops[label] - begin)
        rows = points[chosen].astype(jnp.float32)
        centroid_table = lax.dynamic_slice_in_dim(centroids, (label * BS).astype(jnp.int32), BS, 0).astype(jnp.float32)
        cross_products = jnp.dot(rows, centroid_table.T, preferred_element_type=jnp.float32)
        dists = (jnp.sum(rows * rows, axis=1)[:, None] - 2.0 * cross_products + jnp.sum(centroid_table * centroid_table, axis=1)[None, :]) / width
        onehot_assign = jnp.where(live[:, None] & (finals[chosen][:, None] == columns[None, :]), 1.0, 0.0).astype(jnp.float32)
        sums = jnp.dot(onehot_assign.T, rows, preferred_element_type=jnp.float32)
        counts = jnp.sum(onehot_assign, axis=0)
        fresh = (sums + centroid_table) / (counts + 1.0)[:, None]
        where_to = jnp.where(live, chosen, npoints).astype(jnp.int32)
        return dists.astype(jnp.bfloat16), where_to, fresh

    dists, where_to, fresh = lax.map(one_block, labels)
    table = jnp.zeros((npoints + 1, BS), jnp.bfloat16).at[where_to.reshape(-1)].set(dists.reshape(-1, BS))
    return table[:npoints], fresh.reshape(nblocks * BS, width)
```

```python
import jax
import jax.numpy as jnp
from jax import lax
from jax.sharding import PartitionSpec as P

BS = 256


def block_work(received_points, wanted, centroid_table, width, block_size):
    cent_norm = jnp.sum(jnp.square(centroid_table.astype(jnp.float32)), axis=-1)
    row_norm = jnp.sum(jnp.square(received_points.astype(jnp.float32)), axis=-1)
    cross_products = jnp.einsum(
        "nzy,nvy->nzv", received_points, centroid_table, preferred_element_type=jnp.float32
    )
    dists = ((row_norm[:, :, None] - 2.0 * cross_products + cent_norm[:, None, :]) / width).astype(
        jnp.bfloat16
    )
    onehot_assign = wanted[:, :, None] == jnp.arange(block_size, dtype=jnp.int32)[None, None, :]
    sums = jnp.einsum(
        "xnt,xni->xti",
        onehot_assign.astype(jnp.bfloat16),
        received_points,
        preferred_element_type=jnp.float32,
    )
    counts = jnp.sum(onehot_assign.astype(jnp.float32), axis=1)
    return (dists, sums, counts)


def shards(points, blocks, finals, centroids):
    n_dev = lax.axis_size("dev")
    n_grp = lax.axis_size("grp")
    halves = 2 if n_dev % 2 == 0 else 1
    team = n_dev // halves
    groups = [[h * team + s for s in range(team)] for h in range(halves)]
    swap = [(d, (d + team) % n_dev) for d in range(n_dev)]
    half = lax.axis_index("dev") // team
    npoints, width = points.shape
    block_size = BS
    rows = centroids.shape[0]
    owned = rows // block_size
    nblocks = owned * n_dev
    depth = 2 * npoints // nblocks
    share = width // n_grp
    part = rows // n_grp
    me_grp = lax.axis_index("grp")

    mine = lax.dynamic_slice_in_dim(centroids, me_grp * part, part, 0)
    crossed = lax.ppermute(mine, "dev", swap)
    others = lax.all_gather(crossed, "grp", axis=0, tiled=True)

    block_ids = blocks[:, 0]
    labels = jnp.arange(nblocks, dtype=jnp.int32)
    member = block_ids[:, None] == labels[None, :]
    lower = (jnp.arange(npoints)[:, None] > jnp.arange(npoints)[None, :]).astype(jnp.bfloat16)
    before = jnp.dot(lower, member.astype(jnp.bfloat16), preferred_element_type=jnp.float32)
    ranks = jnp.sum(jnp.where(member, before, 0.0), axis=1).astype(jnp.int32)
    holder = block_ids // owned
    other = (holder // team) ^ half if halves == 2 else 0
    place = ((holder % team) * halves + other) * owned + block_ids % owned
    slots = place * depth + ranks
    outgoing = jnp.zeros((nblocks * depth, width), jnp.bfloat16).at[slots].set(points)
    targets = jnp.full((nblocks * depth,), -1, jnp.int32).at[slots].set(finals)
    outgoing = outgoing.reshape(nblocks, depth, width)
    targets = targets.reshape(nblocks, depth)

    def exchange(x, split, join):
        return lax.all_to_all(
            x, "dev", split_axis=split, concat_axis=join, tiled=True, axis_index_groups=groups
        )

    received_points, wanted = exchange(outgoing, 0, 1), exchange(targets, 0, 1)
    table = jnp.concatenate([centroids, others], axis=0) if halves == 2 else centroids
    table = table.reshape(halves * owned, block_size, width)
    dists, sums, counts = block_work(received_points, wanted, table, width, block_size)
    returned = exchange(dists, 1, 0)
    distances = returned.reshape(nblocks * depth, block_size)[slots]
    sums = sums.reshape(halves * rows, width).astype(jnp.bfloat16)
    counts = counts.reshape(halves * rows)
    if halves == 2:
        far = lax.psum_scatter(sums[rows:], "grp", scatter_dimension=1, tiled=True)
        far = lax.ppermute(far, "dev", swap)
        near = lax.psum_scatter(sums[:rows], "grp", scatter_dimension=1, tiled=True)
        col_sums = near.astype(jnp.float32) + far.astype(jnp.float32)
        all_counts = lax.psum(counts, "grp")
        all_counts = all_counts[:rows] + lax.ppermute(all_counts[rows:], "dev", swap)
    else:
        col_sums = lax.psum_scatter(sums, "grp", scatter_dimension=1, tiled=True).astype(jnp.float32)
        all_counts = lax.psum(counts, "grp")
    own_cols = lax.dynamic_slice_in_dim(centroids, me_grp * share, share, 1).astype(jnp.float32)
    refreshed_centroids = (col_sums + own_cols) / (all_counts + 1.0)[:, None]
    return (distances, refreshed_centroids)


def solution(mesh):
    placed = (P(("grp", "dev"), None), P(("grp", "dev"), None), P(("grp", "dev")), P("dev", None))
    return jax.shard_map(
        shards,
        mesh=mesh,
        in_specs=placed,
        out_specs=(P(("grp", "dev"), None), P("dev", "grp")),
        check_vma=False,
    )
```

```python
import functools

import jax
import jax.numpy as jnp
from jax import lax
from jax.experimental import pallas as pl
from jax.experimental.pallas import tpu as pltpu
from jax.sharding import PartitionSpec as P

BS = 256
MESH = pl.DeviceIdType.MESH
F32, BF16 = jnp.float32, jnp.bfloat16


def kernel(
    n_grp, n_dev, owned, depth,
    slot_row, slot_col, final_row, points, cent, cn_own,
    distances, col_sums, counts_out,
    out, recv, tgt_out, tgt_in, tgt_col, others, cn_oth,
    part, pair_in, x_in, fin, mid_in, dist, ret,
    cnt, cnt_in, cnt_fin, cnt_mid,
    s_pts, r_pts, s_tgt, r_tgt, s_cen, r_cen, s_fwd, r_fwd, s_cn, r_cn,
    s_pair, r_pair, s_x, r_x, s_mid, r_mid, s_cnt, r_cnt, s_cm, r_cm, s_ret, r_ret, l_sem,
):
    team = n_dev // 2
    n_x = n_grp // 2
    g, d = lax.axis_index("grp"), lax.axis_index("dev")
    x, c = g // 2, g % 2
    half, me = d // team, d % team
    npts, width = points.shape
    rows = cent.shape[0]
    share = width // n_grp
    piece = rows // n_grp
    n_cut = 2
    pc = piece // n_cut
    per = owned * depth
    tile = min(256, per)
    nb = tile // depth

    def to(gg, dd):
        return {"grp": gg, "dev": dd}

    def mate(o):
        return half * team + (me + o) % team

    def copy(src, dst, ss, rs, dev):
        return pltpu.make_async_remote_copy(
            src_ref=src, dst_ref=dst, send_sem=ss, recv_sem=rs, device_id=dev, device_id_type=MESH
        )

    swap = to(g, (d + team) % n_dev)
    barrier = pltpu.get_barrier_semaphore()
    peers = [to(g, mate(o)) for o in range(1, team)] + [swap]
    peers += [to((g + o) % n_grp, d) for o in range(1, n_grp)]
    for p in peers:
        pl.semaphore_signal(barrier, inc=1, device_id=p, device_id_type=MESH)
    pl.semaphore_wait(barrier, len(peers))

    def span(gg, j):
        return pl.ds(pl.multiple_of(gg * piece + j * pc, pc), pc)

    cen = [copy(cent.at[span(g, j)], others.at[span(g, j)], s_cen.at[j], r_cen.at[j], swap) for j in range(n_cut)]
    cnc = copy(cn_own, cn_oth, s_cn.at[0], r_cn.at[0], swap)
    for j in range(n_cut):
        cen[j].start()
    cnc.start()

    fwd = [
        copy(others.at[span(g, j)], others.at[span(g, j)], s_fwd.at[j, o], r_fwd.at[j, o], to((g + o) % n_grp, d))
        for j in range(n_cut)
        for o in range(1, n_grp)
    ]

    def packed(h, who, t):
        base = ((who * 2 + h) * owned) * depth + t * tile
        hot = (lax.broadcasted_iota(jnp.int32, (tile, npts), 0) + base == slot_row[...]).astype(BF16)
        pts = jnp.dot(hot, points[...], preferred_element_type=F32).astype(BF16)
        tg = lax.dot_general(final_row[...], hot, (((1,), (1,)), ((), ())), preferred_element_type=F32)
        return pts.reshape(nb, depth, width), tg

    mine = pl.ds(pl.multiple_of(me * depth, depth), depth)
    pts_c, tgt_c = {}, {}
    for h in (1, 0):
        for o in range(1, team):
            pts_c[h, o] = copy(out.at[h, o - 1], recv.at[h, :, mine], s_pts.at[h, o], r_pts.at[h, o], to(g, mate(o)))
            tgt_c[h, o] = copy(tgt_out.at[h, o - 1], tgt_in.at[h, o - 1], s_tgt.at[h, o], r_tgt.at[h, o], to(g, mate(o)))

    def pack_all(h):
        for o in range(1, team):
            for t in range(per // tile):
                pts, tg = packed(h, (me + o) % team, t)
                out[h, o - 1, t * nb : (t + 1) * nb] = pts
                tgt_out[h, o - 1, :, t * tile : (t + 1) * tile] = tg
            pts_c[h, o].start()
            tgt_c[h, o].start()

    def put_targets(h, src, tg):
        col = jnp.transpose(tg)
        tgt_col[h, :, pl.ds(pl.multiple_of(src * depth, depth), depth), :] = col.reshape(-1, depth, 8)

    def pack_own(h):
        for t in range(per // tile):
            pts, tg = packed(h, me, t)
            recv[h, t * nb : (t + 1) * nb, mine] = pts
            tgt_col[h, t * nb : (t + 1) * nb, mine, :] = jnp.transpose(tg).reshape(nb, depth, 8)

    def forward(j):
        cen[j].wait_recv()
        for o in range(1, n_grp):
            fwd[j * (n_grp - 1) + o - 1].start()

    pack_all(1)
    pack_own(1)
    forward(0)
    pack_all(0)
    pack_own(0)
    for j in range(1, n_cut):
        forward(j)

    pair_c = {
        (h, xx): copy(part.at[h, xx * 2 + 1 - c], pair_in.at[h, xx], s_pair.at[h, xx], r_pair.at[h, xx], to(x * 2 + 1 - c, d))
        for h in (1, 0)
        for xx in range(n_x)
    }
    x_c = {
        (h, o): copy(part.at[h, (x + o) % n_x * 2 + c], x_in.at[h, o - 1], s_x.at[h, o], r_x.at[h, o], to((x + o) % n_x * 2 + c, d))
        for h in (1, 0)
        for o in range(1, n_x)
    }
    ret_c = {
        (h, o): copy(dist.at[h, :, pl.ds(pl.multiple_of((me + o) % team * depth, depth), depth)],
                     ret.at[h, me], s_ret.at[h, o], r_ret.at[h, o], to(g, mate(o)))
        for h in (1, 0)
        for o in range(1, team)
    }
    cnt_c = {
        o: copy(cnt, cnt_in.at[o - 1], s_cnt.at[o], r_cnt.at[o], to((g + o) % n_grp, d)) for o in range(1, n_grp)
    }
    mid_c = copy(fin, mid_in, s_mid.at[0], r_mid.at[0], swap)
    cm_c = copy(cnt_fin.at[1], cnt_mid, s_cm.at[0], r_cm.at[0], swap)

    def sums(h):
        for o in range(1, team):
            pts_c[h, o].wait_recv()
            tgt_c[h, o].wait_recv()
            put_targets(h, (me + team - o) % team, tgt_in[h, o - 1])

        @pl.loop(0, owned)
        def _(b):
            want = tgt_col[h, b][:, 0:1].astype(jnp.int32) - 1
            hot = (lax.broadcasted_iota(jnp.int32, (team * depth, BS), 1) == want).astype(F32)
            cnt[h, pl.ds(b, 1), :] = jnp.sum(hot, axis=0, keepdims=True)
            s = lax.dot_general(hot.astype(BF16), recv[h, b], (((0,), (0,)), ((), ())), preferred_element_type=F32)
            s = s.astype(BF16)
            here = pl.ds(pl.multiple_of(b * BS, BS), BS)
            for k in range(n_grp):
                part[h, k, here, :] = s[:, k * share : (k + 1) * share]

        for xx in range(n_x):
            pair_c[h, xx].start()

    def pair(h):
        for xx in range(n_x):
            pair_c[h, xx].wait_recv()
        for o in list(range(1, n_x)) + [0]:
            xx = (x + o) % n_x

            @pl.loop(0, rows // BS)
            def _(b):
                here = pl.ds(pl.multiple_of(b * BS, BS), BS)
                both = part[h, xx * 2 + c, here, :].astype(F32) + pair_in[h, xx, here, :].astype(F32)
                part[h, xx * 2 + c, here, :] = both.astype(BF16)

            if o:
                x_c[h, o].start()

    def dists(h):
        table, norm = (cent, cn_own) if h == 0 else (others, cn_oth)

        @pl.loop(0, owned)
        def _(b):
            pts = recv[h, b]
            tab = table[pl.ds(pl.multiple_of(b * BS, BS), BS), :]
            cross = lax.dot_general(pts, tab, (((1,), (1,)), ((), ())), preferred_element_type=F32)
            wide = pts.astype(F32)
            rn = jnp.sum(wide * wide, axis=1, keepdims=True)
            dist[h, b] = ((rn - 2.0 * cross + norm[pl.ds(b, 1), :]) / width).astype(BF16)

        for o in range(1, team):
            ret_c[h, o].start()
        own = pltpu.make_async_copy(dist.at[h, :, mine], ret.at[h, me], l_sem.at[h])
        own.start()
        own.wait()

    def total(h, here):
        acc = part[h, x * 2 + c, here, :].astype(F32)
        for o in range(1, n_x):
            acc += x_in[h, o - 1, here, :].astype(F32)
        return acc

    sums(1)
    pair(1)
    for j in range(n_cut):
        for o in range(1, n_grp):
            fwd[j * (n_grp - 1) + o - 1].wait_recv()
    cnc.wait_recv()
    dists(1)
    for o in range(1, n_x):
        x_c[1, o].wait_recv()

    @pl.loop(0, rows // BS)
    def _(b):
        here = pl.ds(pl.multiple_of(b * BS, BS), BS)
        fin[here, :] = total(1, here).astype(BF16)

    mid_c.start()
    sums(0)
    for o in range(1, n_grp):
        cnt_c[o].start()
    pair(0)
    dists(0)
    for o in range(1, n_grp):
        cnt_c[o].wait_recv()
    acc = cnt[...]
    for o in range(1, n_grp):
        acc += cnt_in[o - 1]
    cnt_fin[...] = acc
    cm_c.start()
    for h in (1, 0):
        for o in range(1, team):
            ret_c[h, o].wait_recv()

    ptile = min(256, npts)

    @pl.loop(0, npts // ptile)
    def _(t):
        here = pl.ds(pl.multiple_of(t * ptile, ptile), ptile)
        where = slot_col[here, :]
        acc = jnp.zeros((ptile, BS), F32)
        for h in range(2):
            for s in range(team):
                base = (s * 2 + h) * per
                hot = (lax.broadcasted_iota(jnp.int32, (ptile, per), 1) + base == where).astype(BF16)
                acc += jnp.dot(hot, ret[h, s].reshape(per, BS), preferred_element_type=F32)
        distances[here, :] = acc.astype(BF16)

    for o in range(1, n_x):
        x_c[0, o].wait_recv()
    mid_c.wait_recv()

    @pl.loop(0, rows // BS)
    def _(b):
        here = pl.ds(pl.multiple_of(b * BS, BS), BS)
        col_sums[here, :] = total(0, here) + mid_in[here, :].astype(F32)

    cm_c.wait_recv()
    counts_out[...] = cnt_fin[0] + cnt_mid[...]

    for q in cen + [cnc] + fwd + [mid_c, cm_c]:
        q.wait_send()
    for group in (pts_c, tgt_c, pair_c, x_c, ret_c, cnt_c):
        for q in group.values():
            q.wait_send()


def shards(points, blocks, finals, centroids):
    n_dev = lax.axis_size("dev")
    n_grp = lax.axis_size("grp")
    team = n_dev // 2
    half = lax.axis_index("dev") // team
    npoints, width = points.shape
    rows = centroids.shape[0]
    owned = rows // BS
    nblocks = owned * n_dev
    depth = 2 * npoints // nblocks
    share = width // n_grp
    piece = rows // n_grp
    n_x = n_grp // 2
    per = owned * depth

    block_ids = blocks[:, 0]
    labels = jnp.arange(nblocks, dtype=jnp.int32)
    member = block_ids[:, None] == labels[None, :]
    lower = (jnp.arange(npoints)[:, None] > jnp.arange(npoints)[None, :]).astype(BF16)
    before = jnp.dot(lower, member.astype(BF16), preferred_element_type=F32)
    ranks = jnp.sum(jnp.where(member, before, 0.0), axis=1).astype(jnp.int32)
    holder = block_ids // owned
    other = (holder // team) ^ half
    place = ((holder % team) * 2 + other) * owned + block_ids % owned
    slots = place * depth + ranks
    final_row = jnp.broadcast_to((finals + 1).astype(BF16)[None, :], (8, npoints))
    cn = jnp.sum(jnp.square(centroids.astype(F32)), axis=-1).reshape(owned, BS)

    dma = pltpu.SemaphoreType.DMA
    vm = pltpu.VMEM
    distances, col_sums, counts = pl.pallas_call(
        functools.partial(kernel, n_grp, n_dev, owned, depth),
        out_shape=(
            jax.ShapeDtypeStruct((npoints, BS), BF16),
            jax.ShapeDtypeStruct((rows, share), F32),
            jax.ShapeDtypeStruct((owned, BS), F32),
        ),
        in_specs=[pl.BlockSpec(memory_space=vm)] * 6,
        out_specs=(pl.BlockSpec(memory_space=vm),) * 3,
        scratch_shapes=[
            vm((2, team - 1, owned, depth, width), BF16),
            vm((2, owned, team * depth, width), BF16),
            vm((2, team - 1, 8, per), F32),
            vm((2, team - 1, 8, per), F32),
            vm((2, owned, team * depth, 8), F32),
            vm((rows, width), BF16),
            vm((owned, BS), F32),
            vm((2, n_grp, rows, share), BF16),
            vm((2, n_x, rows, share), BF16),
            vm((2, max(n_x - 1, 1), rows, share), BF16),
            vm((rows, share), BF16),
            vm((rows, share), BF16),
            vm((2, owned, team * depth, BS), BF16),
            vm((2, team, owned, depth, BS), BF16),
            vm((2, owned, BS), F32),
            vm((n_grp - 1, 2, owned, BS), F32),
            vm((2, owned, BS), F32),
            vm((owned, BS), F32),
            dma((2, team)), dma((2, team)), dma((2, team)), dma((2, team)),
            dma((2,)), dma((2,)), dma((2, n_grp)), dma((2, n_grp)), dma((1,)), dma((1,)),
            dma((2, n_x)), dma((2, n_x)), dma((2, n_x)), dma((2, n_x)),
            dma((1,)), dma((1,)), dma((n_grp,)), dma((n_grp,)), dma((1,)), dma((1,)),
            dma((2, team)), dma((2, team)), dma((2,)),
        ],
        compiler_params=pltpu.CompilerParams(
            collective_id=0, has_side_effects=True, vmem_limit_bytes=67_000_000
        ),
    )(slots[None, :], slots[:, None], final_row, points, centroids, cn)

    own_cols = lax.dynamic_slice_in_dim(centroids, lax.axis_index("grp") * share, share, 1).astype(F32)
    refreshed_centroids = (col_sums + own_cols) / (counts.reshape(rows) + 1.0)[:, None]
    return (distances, refreshed_centroids)


def solution(mesh):
    placed = (P(("grp", "dev"), None), P(("grp", "dev"), None), P(("grp", "dev")), P("dev", None))
    return jax.shard_map(
        shards,
        mesh=mesh,
        in_specs=placed,
        out_specs=(P(("grp", "dev"), None), P("dev", "grp")),
        check_vma=False,
    )
```

```python
import functools

import jax
import jax.numpy as jnp
from jax import lax
from jax.experimental import pallas as pl
from jax.experimental.pallas import tpu as pltpu
from jax.sharding import PartitionSpec as P

BS = 256
MESH = pl.DeviceIdType.MESH
F32, BF16 = jnp.float32, jnp.bfloat16


def kernel(
    n_grp, n_dev, owned, depth,
    place_row, block_row, final_row, points_hbm, cent_hbm, cn_own,
    distances, col_sums, counts_out,
    points, cent, slot_row, slot_col, out, recv, tgt_out, tgt_in, tgt_col, others, cn_oth,
    part, pair_in, x_in, fin, mid_in, dist, ret,
    cnt, cnt_in, cnt_fin, cnt_mid,
    s_pts, r_pts, s_tgt, r_tgt, s_cen, r_cen, s_fwd, r_fwd, s_cn, r_cn,
    s_pair, r_pair, s_x, r_x, s_mid, r_mid, s_cnt, r_cnt, s_cm, r_cm, s_ret, r_ret, l_sem, in_sem,
):
    team = n_dev // 2
    n_x = n_grp // 2
    g, d = lax.axis_index("grp"), lax.axis_index("dev")
    x, c = g // 2, g % 2
    half, me = d // team, d % team
    npts, width = points.shape
    rows = cent.shape[0]
    share = width // n_grp
    piece = rows // n_grp
    n_cut = 2
    pc = piece // n_cut
    per = owned * depth
    tile = min(256, per)
    nb = tile // depth

    def to(gg, dd):
        return {"grp": gg, "dev": dd}

    def mate(o):
        return half * team + (me + o) % team

    def copy(src, dst, ss, rs, dev):
        return pltpu.make_async_remote_copy(
            src_ref=src, dst_ref=dst, send_sem=ss, recv_sem=rs, device_id=dev, device_id_type=MESH
        )

    load_points = pltpu.make_async_copy(points_hbm, points, in_sem.at[0])
    load_cent = pltpu.make_async_copy(cent_hbm, cent, in_sem.at[1])
    load_points.start()

    swap = to(g, (d + team) % n_dev)
    barrier = pltpu.get_barrier_semaphore()
    peers = [to(g, mate(o)) for o in range(1, team)] + [swap]
    peers += [to((g + o) % n_grp, d) for o in range(1, n_grp)]
    for p in peers:
        pl.semaphore_signal(barrier, inc=1, device_id=p, device_id_type=MESH)
    pl.semaphore_wait(barrier, len(peers))

    def span(gg, j):
        return pl.ds(pl.multiple_of(gg * piece + j * pc, pc), pc)

    cen = [copy(cent_hbm.at[span(g, j)], others.at[span(g, j)], s_cen.at[j], r_cen.at[j], swap) for j in range(n_cut)]
    cnc = copy(cn_own, cn_oth, s_cn.at[0], r_cn.at[0], swap)
    for j in range(n_cut):
        cen[j].start()
    cnc.start()
    load_cent.start()

    n_blocks = owned * n_dev
    step = min(256, npts)
    before = (
        lax.broadcasted_iota(jnp.int32, (step, step), 0) < lax.broadcasted_iota(jnp.int32, (step, step), 1)
    ).astype(BF16)
    seen = jnp.zeros((n_blocks, 1), F32)
    for t in range(npts // step):
        here = slice(t * step, (t + 1) * step)
        member = (lax.broadcasted_iota(jnp.int32, (n_blocks, step), 0) == block_row[:, here]).astype(F32)
        prior = jnp.dot(member.astype(BF16), before, preferred_element_type=F32) + seen
        rank = jnp.sum(member * prior, axis=0, keepdims=True)
        seen = seen + jnp.sum(member, axis=1, keepdims=True)
        slot = place_row[:, here] * depth + rank.astype(jnp.int32)
        slot_row[:, here] = slot
        slot_col[here, :] = jnp.transpose(jnp.broadcast_to(slot.astype(F32), (8, step)))
    load_points.wait()

    fwd = [
        copy(others.at[span(g, j)], others.at[span(g, j)], s_fwd.at[j, o], r_fwd.at[j, o], to((g + o) % n_grp, d))
        for j in range(n_cut)
        for o in range(1, n_grp)
    ]

    def packed(h, who, t):
        base = ((who * 2 + h) * owned) * depth + t * tile
        hot = (lax.broadcasted_iota(jnp.int32, (tile, npts), 0) + base == slot_row[...]).astype(BF16)
        pts = jnp.dot(hot, points[...], preferred_element_type=F32).astype(BF16)
        tg = lax.dot_general(final_row[...], hot, (((1,), (1,)), ((), ())), preferred_element_type=F32)
        return pts.reshape(nb, depth, width), tg

    mine = pl.ds(pl.multiple_of(me * depth, depth), depth)
    pts_c, tgt_c = {}, {}
    for h in (1, 0):
        for o in range(1, team):
            pts_c[h, o] = copy(out.at[h, o - 1], recv.at[h, :, mine], s_pts.at[h, o], r_pts.at[h, o], to(g, mate(o)))
            tgt_c[h, o] = copy(tgt_out.at[h, o - 1], tgt_in.at[h, o - 1], s_tgt.at[h, o], r_tgt.at[h, o], to(g, mate(o)))

    def pack_all(h):
        for o in list(range(team // 2, team)) + list(range(1, team // 2)):
            for t in range(per // tile):
                pts, tg = packed(h, (me + o) % team, t)
                out[h, o - 1, t * nb : (t + 1) * nb] = pts
                tgt_out[h, o - 1, :, t * tile : (t + 1) * tile] = tg
            pts_c[h, o].start()
            tgt_c[h, o].start()

    def put_targets(h, src, tg):
        col = jnp.transpose(tg)
        tgt_col[h, :, pl.ds(pl.multiple_of(src * depth, depth), depth), :] = col.reshape(-1, depth, 8)

    def pack_own(h):
        for t in range(per // tile):
            pts, tg = packed(h, me, t)
            recv[h, t * nb : (t + 1) * nb, mine] = pts
            tgt_col[h, t * nb : (t + 1) * nb, mine, :] = jnp.transpose(tg).reshape(nb, depth, 8)

    def forward(j):
        cen[j].wait_recv()
        for o in range(1, n_grp):
            fwd[j * (n_grp - 1) + o - 1].start()

    pack_all(1)
    pack_own(1)
    forward(0)
    pack_all(0)
    pack_own(0)
    for j in range(1, n_cut):
        forward(j)

    pair_c = {
        (h, xx): copy(part.at[h, xx * 2 + 1 - c], pair_in.at[h, xx], s_pair.at[h, xx], r_pair.at[h, xx], to(x * 2 + 1 - c, d))
        for h in (1, 0)
        for xx in range(n_x)
    }
    x_c = {
        (h, o): copy(part.at[h, (x + o) % n_x * 2 + c], x_in.at[h, o - 1], s_x.at[h, o], r_x.at[h, o], to((x + o) % n_x * 2 + c, d))
        for h in (1, 0)
        for o in range(1, n_x)
    }
    ret_c = {
        (h, o): copy(dist.at[h, :, pl.ds(pl.multiple_of((me + o) % team * depth, depth), depth)],
                     ret.at[h, me], s_ret.at[h, o], r_ret.at[h, o], to(g, mate(o)))
        for h in (1, 0)
        for o in range(1, team)
    }
    cnt_c = {
        o: copy(cnt, cnt_in.at[o - 1], s_cnt.at[o], r_cnt.at[o], to((g + o) % n_grp, d)) for o in range(1, n_grp)
    }
    mid_c = copy(fin, mid_in, s_mid.at[0], r_mid.at[0], swap)
    cm_c = copy(cnt_fin.at[1], cnt_mid, s_cm.at[0], r_cm.at[0], swap)

    def sums(h):
        for o in range(1, team):
            pts_c[h, o].wait_recv()
            tgt_c[h, o].wait_recv()
            put_targets(h, (me + team - o) % team, tgt_in[h, o - 1])

        @pl.loop(0, owned)
        def _(b):
            want = tgt_col[h, b][:, 0:1].astype(jnp.int32) - 1
            hot = (lax.broadcasted_iota(jnp.int32, (team * depth, BS), 1) == want).astype(F32)
            cnt[h, pl.ds(b, 1), :] = jnp.sum(hot, axis=0, keepdims=True)
            s = lax.dot_general(hot.astype(BF16), recv[h, b], (((0,), (0,)), ((), ())), preferred_element_type=F32)
            s = s.astype(BF16)
            here = pl.ds(pl.multiple_of(b * BS, BS), BS)
            for k in range(n_grp):
                part[h, k, here, :] = s[:, k * share : (k + 1) * share]

        for xx in range(n_x):
            pair_c[h, xx].start()

    def pair(h):
        for xx in range(n_x):
            pair_c[h, xx].wait_recv()
        for o in list(range(1, n_x)) + [0]:
            xx = (x + o) % n_x

            @pl.loop(0, rows // BS)
            def _(b):
                here = pl.ds(pl.multiple_of(b * BS, BS), BS)
                both = part[h, xx * 2 + c, here, :].astype(F32) + pair_in[h, xx, here, :].astype(F32)
                part[h, xx * 2 + c, here, :] = both.astype(BF16)

            if o:
                x_c[h, o].start()

    def dists(h):
        table, norm = (cent, cn_own) if h == 0 else (others, cn_oth)

        @pl.loop(0, owned)
        def _(b):
            pts = recv[h, b]
            tab = table[pl.ds(pl.multiple_of(b * BS, BS), BS), :]
            cross = lax.dot_general(pts, tab, (((1,), (1,)), ((), ())), preferred_element_type=F32)
            wide = pts.astype(F32)
            rn = jnp.sum(wide * wide, axis=1, keepdims=True)
            dist[h, b] = ((rn - 2.0 * cross + norm[pl.ds(b, 1), :]) / width).astype(BF16)

        for o in range(1, team):
            ret_c[h, o].start()
        own = pltpu.make_async_copy(dist.at[h, :, mine], ret.at[h, me], l_sem.at[h])
        own.start()
        own.wait()

    def total(h, here):
        acc = part[h, x * 2 + c, here, :].astype(F32)
        for o in range(1, n_x):
            acc += x_in[h, o - 1, here, :].astype(F32)
        return acc

    load_cent.wait()
    sums(1)
    pair(1)
    for j in range(n_cut):
        for o in range(1, n_grp):
            fwd[j * (n_grp - 1) + o - 1].wait_recv()
    cnc.wait_recv()
    dists(1)
    for o in range(1, n_x):
        x_c[1, o].wait_recv()

    @pl.loop(0, rows // BS)
    def _(b):
        here = pl.ds(pl.multiple_of(b * BS, BS), BS)
        fin[here, :] = total(1, here).astype(BF16)

    mid_c.start()
    sums(0)
    for o in range(1, n_grp):
        cnt_c[o].start()
    dists(0)
    pair(0)
    for o in range(1, n_grp):
        cnt_c[o].wait_recv()
    acc = cnt[...]
    for o in range(1, n_grp):
        acc += cnt_in[o - 1]
    cnt_fin[...] = acc
    cm_c.start()
    ptile = min(256, npts)

    def gather(h):
        for o in range(1, team):
            ret_c[h, o].wait_recv()

        @pl.loop(0, npts // ptile)
        def _(t):
            here = pl.ds(pl.multiple_of(t * ptile, ptile), ptile)
            where = slot_col[here, 0:1].astype(jnp.int32)
            acc = jnp.zeros((ptile, BS), F32)
            for s in range(team):
                base = (s * 2 + h) * per
                hot = (lax.broadcasted_iota(jnp.int32, (ptile, per), 1) + base == where).astype(BF16)
                acc += jnp.dot(hot, ret[h, s].reshape(per, BS), preferred_element_type=F32)
            if h == 0:
                acc += distances[here, :].astype(F32)
            distances[here, :] = acc.astype(BF16)

    gather(1)
    gather(0)
    for o in range(1, n_x):
        x_c[0, o].wait_recv()
    mid_c.wait_recv()

    @pl.loop(0, rows // BS)
    def _(b):
        here = pl.ds(pl.multiple_of(b * BS, BS), BS)
        col_sums[here, :] = total(0, here) + mid_in[here, :].astype(F32)

    cm_c.wait_recv()
    counts_out[...] = cnt_fin[0] + cnt_mid[...]

    for q in cen + [cnc] + fwd + [mid_c, cm_c]:
        q.wait_send()
    for group in (pts_c, tgt_c, pair_c, x_c, ret_c, cnt_c):
        for q in group.values():
            q.wait_send()


def shards(points, blocks, finals, centroids):
    n_dev = lax.axis_size("dev")
    n_grp = lax.axis_size("grp")
    team = n_dev // 2
    half = lax.axis_index("dev") // team
    npoints, width = points.shape
    rows = centroids.shape[0]
    owned = rows // BS
    nblocks = owned * n_dev
    depth = 2 * npoints // nblocks
    share = width // n_grp
    piece = rows // n_grp
    n_x = n_grp // 2
    per = owned * depth

    block_ids = blocks[:, 0]
    holder = block_ids // owned
    other = (holder // team) ^ half
    place = ((holder % team) * 2 + other) * owned + block_ids % owned
    final_row = jnp.broadcast_to((finals + 1).astype(BF16)[None, :], (8, npoints))
    cn = jnp.sum(jnp.square(centroids.astype(F32)), axis=-1).reshape(owned, BS)

    dma = pltpu.SemaphoreType.DMA
    vm = pltpu.VMEM
    distances, col_sums, counts = pl.pallas_call(
        functools.partial(kernel, n_grp, n_dev, owned, depth),
        out_shape=(
            jax.ShapeDtypeStruct((npoints, BS), BF16),
            jax.ShapeDtypeStruct((rows, share), F32),
            jax.ShapeDtypeStruct((owned, BS), F32),
        ),
        in_specs=[pl.BlockSpec(memory_space=vm)] * 3
        + [pl.BlockSpec(memory_space=pl.ANY)] * 2
        + [pl.BlockSpec(memory_space=vm)],
        out_specs=(pl.BlockSpec(memory_space=vm),) * 3,
        scratch_shapes=[
            vm((npoints, width), BF16),
            vm((rows, width), BF16),
            vm((1, npoints), jnp.int32),
            vm((npoints, 8), F32),
            vm((2, team - 1, owned, depth, width), BF16),
            vm((2, owned, team * depth, width), BF16),
            vm((2, team - 1, 8, per), F32),
            vm((2, team - 1, 8, per), F32),
            vm((2, owned, team * depth, 8), F32),
            vm((rows, width), BF16),
            vm((owned, BS), F32),
            vm((2, n_grp, rows, share), BF16),
            vm((2, n_x, rows, share), BF16),
            vm((2, max(n_x - 1, 1), rows, share), BF16),
            vm((rows, share), BF16),
            vm((rows, share), BF16),
            vm((2, owned, team * depth, BS), BF16),
            vm((2, team, owned, depth, BS), BF16),
            vm((2, owned, BS), F32),
            vm((n_grp - 1, 2, owned, BS), F32),
            vm((2, owned, BS), F32),
            vm((owned, BS), F32),
            dma((2, team)), dma((2, team)), dma((2, team)), dma((2, team)),
            dma((2,)), dma((2,)), dma((2, n_grp)), dma((2, n_grp)), dma((1,)), dma((1,)),
            dma((2, n_x)), dma((2, n_x)), dma((2, n_x)), dma((2, n_x)),
            dma((1,)), dma((1,)), dma((n_grp,)), dma((n_grp,)), dma((1,)), dma((1,)),
            dma((2, team)), dma((2, team)), dma((2,)), dma((2,)),
        ],
        compiler_params=pltpu.CompilerParams(
            collective_id=0, has_side_effects=True, vmem_limit_bytes=67_000_000
        ),
    )(place[None, :], block_ids[None, :], final_row, points, centroids, cn)

    own_cols = lax.dynamic_slice_in_dim(centroids, lax.axis_index("grp") * share, share, 1).astype(F32)
    refreshed_centroids = (col_sums + own_cols) / (counts.reshape(rows) + 1.0)[:, None]
    return (distances, refreshed_centroids)


def solution(mesh):
    placed = (P(("grp", "dev"), None), P(("grp", "dev"), None), P(("grp", "dev")), P("dev", None))
    return jax.shard_map(
        shards,
        mesh=mesh,
        in_specs=placed,
        out_specs=(P(("grp", "dev"), None), P("dev", "grp")),
        check_vma=False,
    )
```
